32 devices in a mesh: grp: 2 (over y), seq: 4 (over z), head: 2 (over x), rep: 2 (over core).
Axes of the slice: x: 2, y: 2, z: 4, core: 2. Of those that a mesh axis runs over, the one named last changes fastest.
Arguments:
- queries: bfloat16 [16, 4096], P(('grp', 'rep'), 'head'), parts along dimension 0, may hold values from -6 to 6
- k_cache: bfloat16 [16, 16, 4096, 128], P(('grp', 'rep'), 'head', 'seq'), parts along dimension 0, may hold values from -6 to 6
- v_cache: bfloat16 [16, 16, 4096, 128], P(('grp', 'rep'), 'head', 'seq'), parts along dimension 0, may hold values from -6 to 6
- page_table: int32 [16, 32], P(('grp', 'rep')), parts along dimension 0, may hold values from 0 to 31, each once within a row
- lengths: int32 [16], P(('grp', 'rep')), parts along dimension 0, may hold values from 512 to 4096
- keep_threshold: int32 [16, 16], P(('grp', 'rep'), 'head'), parts along dimension 0, may hold values from 256 to 8191
Outputs:
- attended: bfloat16 [16, 4096], P(('grp', 'rep'), 'head'), parts along dimension 0
- token_mass: float32 [16, 16, 4096], P(('grp', 'rep'), 'head', 'seq'), parts along dimension 0
- page_keep: float32 [16, 16, 32], P(('grp', 'rep'), 'head', 'seq'), parts along dimension 0
The draws below stay inside these ranges and needn't reach their ends.
There are 2 independent parts, one for each index of `grp`. The reference program is written for one: setup_inputs(seed, part) draws one part's arguments, and reference() takes and returns one part's arrays. A program takes and returns all parts, laid end to end along the dimension named above; each array names one. Nothing has to cross between parts.
Inputs may be any that keep to these rules, and one draw needn't show every extreme that they name: `page_table`: each row names every physical page slot 0 to 31 once.
All inputs are finite; a program needn't handle non-finite values.
Results may differ from the reference program's by a relative error of at most 0.0052.
Values sent between devices are 32-bit elements; how exact they have to be, the bound alone decides.
No kernel may reach another device: no remote copies, remote signals or barrier semaphores. Data moves between devices by JAX's collectives and lax.ppermute only.
A program may use at most 64 MiB of HBM per device.

```python
import jax
import jax.numpy as jnp
from jax import lax

QH = 32
KVH = 16
HD = 128
PAGE = 128
BATCH = 8
PAGES = 32
CTX = 4096


def set_ends(drawn, own_key, smallest, top_value):
    index_at = [jax.random.randint(jax.random.fold_in(own_key, axis), (), 0, length) for axis, length in enumerate(drawn.shape)]
    longest = drawn.shape.index(max(drawn.shape))
    neighbour = index_at[:longest] + [(index_at[longest] + 1) % drawn.shape[longest]] + index_at[longest + 1:]
    return drawn.at[tuple(index_at)].set(smallest).at[tuple(neighbour)].set(top_value)


def block_levels(rng, extent, shards, smallest, top_value):
    def one(dim, blocks):
        steps = jax.random.uniform(jax.random.fold_in(jax.random.fold_in(rng, 6), dim), (blocks,), jnp.float32, smallest / len(shards), top_value / len(shards))
        return jnp.repeat(jnp.exp(steps), extent[dim] // blocks).reshape((-1,) + (1,) * (len(extent) - dim - 1))

    gain = one(*shards[0])
    for cut in shards[1:]:
        gain = gain * one(*cut)
    return gain


def centred(own_key, shape, scale, bound, cuts=(), kind=jnp.bfloat16):
    gain = block_levels(own_key, shape, cuts, -0.22, 0.18) if cuts else 1.0
    result = jax.random.normal(own_key, shape, jnp.float32) * scale * gain
    return jnp.minimum(jnp.maximum(result, -bound), bound).astype(kind)


def setup_inputs(seed: int = 0, part: int = 0) -> dict:
    arg_keys = jax.random.split(jax.random.key(seed), 7)
    part_splits = jax.random.split(jax.random.fold_in(arg_keys[6], part), 7)
    return {
        "queries": centred(part_splits[0], (BATCH, QH * HD), 1.0, 6.0, ((0, 2), (1, 2))),
        "k_cache": centred(part_splits[1], (BATCH, KVH, CTX, HD), 1.0, 6.0, ((0, 2), (1, 2), (2, 4))),
        "v_cache": centred(part_splits[2], (BATCH, KVH, CTX, HD), 1.0, 6.0, ((0, 2), (1, 2), (2, 4))),
        "page_table": jax.vmap(lambda own: jax.random.permutation(own, PAGES))(jax.random.split(part_splits[3], BATCH)).reshape((BATCH, PAGES)).astype(jnp.int32),
        "lengths": set_ends(jax.random.randint(part_splits[4], (BATCH,), CTX // 8, CTX + 1), jax.random.fold_in(part_splits[4], 1), CTX // 8, CTX).astype(jnp.int32),
        "keep_threshold": set_ends(jax.random.randint(part_splits[5], (BATCH, KVH), 256, 8192), jax.random.fold_in(part_splits[5], 1), 256, 8191).astype(jnp.int32),
    }


softcap = 50.0
query_scale = 1.0 / 12.0
quanta = 65536.0


def one_request(inputs):
    query_row, keys_all, values_all, table_row, length_one, threshold_row = inputs
    group = QH // KVH
    slots = (table_row[:, None] * PAGE + jnp.arange(PAGE, dtype=jnp.int32)[None, :]).reshape(-1).astype(jnp.int32)
    keys_logical = keys_all[:, slots, :].astype(jnp.float32)
    values_logical = values_all[:, slots, :].astype(jnp.float32)
    grouped = query_row.reshape(KVH, group, HD).astype(jnp.float32)
    logits = jnp.einsum("kgd,ktd->kgt", grouped, keys_logical)
    capped = softcap * jnp.tanh(logits * query_scale / softcap)
    is_live = jnp.arange(CTX, dtype=jnp.int32) < length_one
    weights = jnp.where(is_live[None, None, :], jnp.exp(capped - softcap), jnp.float32(0.0))
    denom = jnp.sum(weights, axis=2)
    numer = jnp.einsum("kgt,ktd->kgd", weights.astype(jnp.bfloat16).astype(jnp.float32), values_logical)
    attended = (numer / denom[:, :, None]).astype(jnp.bfloat16).reshape(QH * HD)
    token_mass = jnp.sum(weights / denom[:, :, None], axis=1)
    page_mass = jnp.sum(token_mass.reshape(KVH, PAGES, PAGE), axis=2)
    page_keep = jnp.minimum(jnp.float32(1.0), quanta * page_mass / threshold_row.astype(jnp.float32)[:, None])
    return attended, token_mass, page_keep


def reference(queries, k_cache, v_cache, page_table, lengths, keep_threshold):
    attended, token_mass, page_keep = lax.map(one_request, (queries, k_cache, v_cache, page_table, lengths, keep_threshold))
    return (attended, token_mass, page_keep)
```

```python
import jax
import jax.numpy as jnp
from jax import lax
from jax.experimental import pallas as pl
from jax.experimental.pallas import tpu as pltpu
from jax.sharding import PartitionSpec as P

PAGE = 128

softcap = 50.0
query_scale = 1.0 / 12.0
quanta = 65536.0


def pick_row(rows, r):
    at = lax.broadcasted_iota(jnp.int32, rows.shape, 0) == r
    return jnp.sum(jnp.where(at, rows, 0.0), axis=0, keepdims=True)


def score_kernel(lengths, table, queries, keys, weights, denom):
    r, t = pl.program_id(0), pl.program_id(1)
    kv, tok, hd = keys.shape[1:]
    heads = weights.shape[1]
    group = heads // kv
    pages = tok // PAGE
    first = (lax.axis_index("seq") * pl.num_programs(1) + t) * pages

    row = pick_row(queries[...].astype(jnp.float32), r)
    stack = [row[:, (k * group + g) * hd:(k * group + g + 1) * hd] for g in range(group) for k in range(kv)]
    q = jnp.concatenate(stack, axis=0).astype(jnp.bfloat16)
    head = lax.broadcasted_iota(jnp.int32, (heads, tok), 0) % kv
    logits = jnp.zeros((heads, tok), jnp.float32)
    for k in range(kv):
        one = lax.dot_general(q, keys[0, k], (((1,), (1,)), ((), ())), preferred_element_type=jnp.float32)
        logits = jnp.where(head == k, one, logits)
    value = jnp.exp(softcap * jnp.tanh(logits * query_scale / softcap) - softcap)

    slots = pick_row(table[...].astype(jnp.float32), r)
    order = lax.broadcasted_iota(jnp.int32, slots.shape, 1).astype(jnp.float32)
    lane = lax.broadcasted_iota(jnp.int32, (heads, PAGE), 1).astype(jnp.float32)
    length = lengths[r].astype(jnp.float32)
    total = jnp.zeros((heads, PAGE), jnp.float32)
    for i in range(pages):
        here = slots == (first + i).astype(jnp.float32)
        logical = jnp.sum(jnp.where(here, order, 0.0), axis=1, keepdims=True)
        live = lane + logical * PAGE < length
        piece = jnp.where(live, value[:, i * PAGE:(i + 1) * PAGE], 0.0)
        weights[0, :, i * PAGE:(i + 1) * PAGE] = piece
        total = total + piece
    total = jnp.broadcast_to(jnp.sum(total, axis=1, keepdims=True), total.shape)

    @pl.when(t == 0)
    def _():
        denom[0] = total

    @pl.when(t > 0)
    def _():
        denom[0] += total


def value_kernel(weights, values, numer):
    t = pl.program_id(1)
    kv = values.shape[1]
    heads = weights.shape[1]
    w = weights[0].astype(jnp.bfloat16)
    out = jnp.zeros(numer.shape[1:], jnp.float32)
    head = lax.broadcasted_iota(jnp.int32, out.shape, 0) % kv
    for k in range(kv):
        one = jnp.dot(w, values[0, k], preferred_element_type=jnp.float32)
        out = jnp.where(head == k, one, out)

    @pl.when(t == 0)
    def _():
        numer[0] = out

    @pl.when(t > 0)
    def _():
        numer[0] += out


def mass_kernel(*refs):
    weights, numer = refs[:2]
    denoms, out = refs[2:-1], refs[-1]
    requests, heads, tok = weights.shape
    kv = out.shape[1]
    for r in range(requests):
        denom = sum(d[r] for d in denoms)
        for i in range(tok // PAGE):
            share = weights[r, :, i * PAGE:(i + 1) * PAGE] / denom
            out[r, :, i * PAGE:(i + 1) * PAGE] = sum(share[g:g + kv] for g in range(0, heads, kv))
        for g in range(heads // kv):
            at = tok + g * PAGE
            out[r, :, at:at + PAGE] = numer[r, g * kv:(g + 1) * kv, :]


def finish_kernel(table, threshold, *refs):
    ranks = (len(refs) - 4) // 2
    denoms, pieces = refs[:ranks], refs[ranks:2 * ranks]
    attended, mass, keep, rows = refs[2 * ranks:]
    requests, kv, tok = mass.shape
    pages = tok // PAGE
    seq = lax.axis_index("seq")
    group = (pieces[0].shape[2] - tok) // PAGE
    lane = lax.broadcasted_iota(jnp.int32, (kv, pages), 1)
    eye = lax.broadcasted_iota(jnp.int32, (kv, kv), 0) == lax.broadcasted_iota(jnp.int32, (kv, kv), 1)
    for r in range(requests):
        sums = jnp.zeros((kv, pages), jnp.float32)
        for m in range(pages):
            slot = table[r, seq * pages + m]
            away = seq - slot // pages
            away = jnp.where(away < 0, away + ranks, away)
            at = pl.multiple_of(slot % pages * PAGE, PAGE)
            page = pieces[0][r, :, pl.ds(at, PAGE)]
            for b in range(1, ranks):
                page = jnp.where(away == b, pieces[b][r, :, pl.ds(at, PAGE)], page)
            mass[r, :, m * PAGE:(m + 1) * PAGE] = page
            sums = jnp.where(lane == m, jnp.sum(page, axis=1, keepdims=True), sums)
        bar = threshold[r:r + 1, :].astype(jnp.float32)
        bar = jnp.sum(jnp.where(eye, bar, 0.0), axis=1, keepdims=True)
        keep[r] = jnp.minimum(1.0, quanta * sums / bar)
        denom = sum(d[r] for d in denoms)
        for g in range(group):
            at = tok + g * PAGE
            numer = sum(p[r, :, at:at + PAGE] for p in pieces)
            ratio = numer / denom[g * kv:(g + 1) * kv]
            for k in range(kv):
                h = k * group + g
                rows[r:r + 1, h * PAGE:(h + 1) * PAGE] = ratio[k:k + 1]
    attended[...] = rows[...].astype(attended.dtype)


def program(ranks):
    def spread(x):
        rings = [[(i, (i + s) % ranks) for i in range(ranks)] for s in range(1, ranks)]
        return [x] + [lax.ppermute(x, "seq", ring) for ring in rings]

    def shards(queries, k_cache, v_cache, page_table, lengths, keep_threshold):
        requests, kv, tok, hd = k_cache.shape
        heads = queries.shape[1] // hd
        group = heads // kv
        pages = tok // PAGE
        steps = 2 if pages % 2 == 0 else 1
        part = tok // steps
        flops = 2 * requests * heads * tok * hd
        cost = pl.CostEstimate(flops=flops * 64, bytes_accessed=2 * k_cache.size, transcendentals=0)
        smem = pl.BlockSpec(memory_space=pltpu.SMEM)
        vmem = pl.BlockSpec(memory_space=pltpu.VMEM)
        cache = pl.BlockSpec((1, kv, part, hd), lambda r, t: (r, 0, t, 0))
        w_block = pl.BlockSpec((1, heads, part), lambda r, t: (r, 0, t))
        small = pl.BlockSpec((1, heads, PAGE), lambda r, t: (r, 0, 0))
        small_shape = jax.ShapeDtypeStruct((requests, heads, PAGE), jnp.float32)
        weights, denom = pl.pallas_call(
            score_kernel,
            grid=(requests, steps),
            in_specs=[smem, vmem, vmem, cache],
            out_specs=[w_block, small],
            out_shape=[jax.ShapeDtypeStruct((requests, heads, tok), jnp.float32), small_shape],
            cost_estimate=cost,
            name="score",
        )(lengths, page_table, queries, k_cache)
        denoms = spread(denom)
        numer = pl.pallas_call(
            value_kernel,
            grid=(requests, steps),
            in_specs=[w_block, cache],
            out_specs=small,
            out_shape=small_shape,
            cost_estimate=cost,
            name="value",
        )(weights, v_cache)
        piece = pl.pallas_call(
            mass_kernel,
            in_specs=[vmem] * (2 + ranks),
            out_specs=vmem,
            out_shape=jax.ShapeDtypeStruct((requests, kv, tok + group * PAGE), jnp.float32),
            name="mass",
        )(weights, numer, *denoms)
        pieces = spread(piece)
        return pl.pallas_call(
            finish_kernel,
            in_specs=[smem, vmem] + [vmem] * (2 * ranks),
            out_specs=[vmem, vmem, vmem],
            out_shape=[
                jax.ShapeDtypeStruct((requests, heads * hd), jnp.bfloat16),
                jax.ShapeDtypeStruct((requests, kv, tok), jnp.float32),
                jax.ShapeDtypeStruct((requests, kv, pages), jnp.float32),
            ],
            scratch_shapes=[pltpu.VMEM((requests, heads * hd), jnp.float32)],
            name="finish",
        )(page_table, keep_threshold, *denoms, *pieces)

    return shards


def solution(mesh):
    placed = (
        P(("grp", "rep"), "head"),
        P(("grp", "rep"), "head", "seq", None),
        P(("grp", "rep"), "head", "seq", None),
        P(("grp", "rep"), None),
        P(("grp", "rep")),
        P(("grp", "rep"), "head"),
    )
    return jax.shard_map(
        program(mesh.shape["seq"]),
        mesh=mesh,
        in_specs=placed,
        out_specs=(
            P(("grp", "rep"), "head"),
            P(("grp", "rep"), "head", "seq"),
            P(("grp", "rep"), "head", "seq"),
        ),
        check_vma=False,
    )
```

```python
import jax
import jax.numpy as jnp
from jax import lax
from jax.experimental import pallas as pl
from jax.experimental.pallas import tpu as pltpu
from jax.sharding import PartitionSpec as P

PAGE = 128

softcap = 50.0
query_scale = 1.0 / 12.0
quanta = 65536.0


def finish_kernel(table, threshold, *refs):
    ranks = len(refs) - 2
    pieces = refs[:ranks]
    mass, keep = refs[ranks:]
    requests, kv, tok = mass.shape
    pages = tok // PAGE
    seq = lax.axis_index("seq")
    lane = lax.broadcasted_iota(jnp.int32, (kv, pages), 1)
    eye = lax.broadcasted_iota(jnp.int32, (kv, kv), 0) == lax.broadcasted_iota(jnp.int32, (kv, kv), 1)
    for r in range(requests):
        sums = jnp.zeros((kv, pages), jnp.float32)
        for m in range(pages):
            slot = table[r, seq * pages + m]
            away = seq - slot // pages
            away = jnp.where(away < 0, away + ranks, away)
            at = pl.multiple_of(slot % pages * PAGE, PAGE)
            page = pieces[0][r, :, pl.ds(at, PAGE)]
            for b in range(1, ranks):
                page = jnp.where(away == b, pieces[b][r, :, pl.ds(at, PAGE)], page)
            mass[r, :, m * PAGE:(m + 1) * PAGE] = page
            sums = jnp.where(lane == m, jnp.sum(page, axis=1, keepdims=True), sums)
        bar = threshold[r:r + 1, :].astype(jnp.float32)
        bar = jnp.sum(jnp.where(eye, bar, 0.0), axis=1, keepdims=True)
        keep[r] = jnp.minimum(1.0, quanta * sums / bar)


def fold(parts):
    while len(parts) > 1:
        half = (len(parts) + 1) // 2
        parts = [a + b for a, b in zip(parts[:half], parts[half:])] + parts[len(parts) - half:half]
    return parts[0]


def program(ranks):
    def spread(x):
        rings = [[(i, (i + s) % ranks) for i in range(ranks)] for s in range(1, ranks)]
        return [x] + [lax.ppermute(x, "seq", ring) for ring in rings]

    def shards(queries, k_cache, v_cache, page_table, lengths, keep_threshold):
        requests, kv, tok, hd = k_cache.shape
        heads = queries.shape[1] // hd
        group = heads // kv
        pages = tok // PAGE
        pages_all = page_table.shape[1]
        slot_ids = lax.axis_index("seq") * pages + jnp.arange(pages, dtype=jnp.int32)
        matches = page_table[:, None, :] == slot_ids[None, :, None]
        order = jnp.arange(pages_all, dtype=jnp.int32)[None, None, :]
        logical = jnp.sum(jnp.where(matches, order, 0), axis=2)
        offset = jnp.arange(PAGE, dtype=jnp.int32)[None, None, :]
        position = (logical[:, :, None] * PAGE + offset).reshape(requests, tok)
        is_live = position < lengths[:, None]
        grouped = queries.reshape(requests, kv, group, hd)
        logits = jnp.einsum("rkgd,rktd->rkgt", grouped, k_cache, preferred_element_type=jnp.float32)
        capped = softcap * jnp.tanh(logits * query_scale / softcap)
        weights = jnp.where(is_live[:, None, None, :], jnp.exp(capped - softcap), 0.0)
        denom = fold(spread(jnp.sum(weights, axis=3)))
        numer = jnp.einsum(
            "rkgt,rktd->rkgd", weights.astype(jnp.bfloat16), v_cache, preferred_element_type=jnp.float32
        )
        numers = spread(numer)
        pieces = spread(jnp.sum(weights / denom[..., None], axis=2))
        attended = (fold(numers) / denom[..., None]).astype(jnp.bfloat16).reshape(requests, heads * hd)
        smem = pl.BlockSpec(memory_space=pltpu.SMEM)
        vmem = pl.BlockSpec(memory_space=pltpu.VMEM)
        mass, keep = pl.pallas_call(
            finish_kernel,
            in_specs=[smem, vmem] + [vmem] * ranks,
            out_specs=[vmem, vmem],
            out_shape=[
                jax.ShapeDtypeStruct((requests, kv, tok), jnp.float32),
                jax.ShapeDtypeStruct((requests, kv, pages), jnp.float32),
            ],
            name="finish",
        )(page_table, keep_threshold, *[pltpu.with_memory_space_constraint(p, pltpu.VMEM) for p in pieces])
        return attended, mass, keep

    return shards


def solution(mesh):
    placed = (
        P(("grp", "rep"), "head"),
        P(("grp", "rep"), "head", "seq", None),
        P(("grp", "rep"), "head", "seq", None),
        P(("grp", "rep"), None),
        P(("grp", "rep")),
        P(("grp", "rep"), "head"),
    )
    return jax.shard_map(
        program(mesh.shape["seq"]),
        mesh=mesh,
        in_specs=placed,
        out_specs=(
            P(("grp", "rep"), "head"),
            P(("grp", "rep"), "head", "seq"),
            P(("grp", "rep"), "head", "seq"),
        ),
        check_vma=False,
    )
```

```python
import jax
import jax.numpy as jnp
from jax import lax
from jax.experimental import pallas as pl
from jax.experimental.pallas import tpu as pltpu
from jax.sharding import PartitionSpec as P


PAGE = 128

softcap = 50.0
query_scale = 1.0 / 12.0
quanta = 65536.0


def finish_kernel(table, threshold, *refs):
    ranks = len(refs) - 2
    pieces = refs[:ranks]
    mass, keep = refs[ranks:]
    requests, kv, tok = mass.shape
    pages = tok // PAGE
    seq = lax.axis_index("seq")
    lane = lax.broadcasted_iota(jnp.int32, (kv, pages), 1)
    eye = lax.broadcasted_iota(jnp.int32, (kv, kv), 0) == lax.broadcasted_iota(jnp.int32, (kv, kv), 1)
    for r in range(requests):
        sums = jnp.zeros((kv, pages), jnp.float32)
        for m in range(pages):
            slot = table[r, seq * pages + m]
            away = seq ^ (slot // pages)
            at = pl.multiple_of(slot % pages * PAGE, PAGE)
            page = pieces[0][r, :, pl.ds(at, PAGE)]
            for b in range(1, ranks):
                page = jnp.where(away == b, pieces[b][r, :, pl.ds(at, PAGE)], page)
            mass[r, :, m * PAGE:(m + 1) * PAGE] = page
            sums = jnp.where(lane == m, jnp.sum(page, axis=1, keepdims=True), sums)
        bar = threshold[r:r + 1, :].astype(jnp.float32)
        bar = jnp.sum(jnp.where(eye, bar, 0.0), axis=1, keepdims=True)
        keep[r] = jnp.minimum(1.0, quanta * sums / bar)


def program(ranks):
    assert ranks & (ranks - 1) == 0
    bits = [1 << b for b in reversed(range(ranks.bit_length() - 1))]

    def swap(x, bit):
        return lax.ppermute(x, "seq", [(i, i ^ bit) for i in range(ranks)])

    def direct_sum(x):
        parts = [x] + [swap(x, s) for s in range(1, ranks)]
        while len(parts) > 1:
            half = len(parts) // 2
            parts = [a + b for a, b in zip(parts[:half], parts[half:])]
        return parts[0]

    def staged_sum(x):
        for bit in bits:
            x = x + swap(x, bit)
        return x

    def spread(x):
        parts = {0: x}
        for bit in bits:
            for s, part in list(parts.items()):
                parts[s ^ bit] = swap(part, bit)
        return [parts[s] for s in range(ranks)]

    def shards(queries, k_cache, v_cache, page_table, lengths, keep_threshold):
        requests, kv, tok, hd = k_cache.shape
        heads = queries.shape[1] // hd
        group = heads // kv
        pages = tok // PAGE
        pages_all = page_table.shape[1]
        slot_ids = lax.axis_index("seq") * pages + jnp.arange(pages, dtype=jnp.int32)
        matches = page_table[:, None, :] == slot_ids[None, :, None]
        order = jnp.arange(pages_all, dtype=jnp.int32)[None, None, :]
        logical = jnp.sum(jnp.where(matches, order, 0), axis=2)
        offset = jnp.arange(PAGE, dtype=jnp.int32)[None, None, :]
        position = (logical[:, :, None] * PAGE + offset).reshape(requests, tok)
        is_live = position < lengths[:, None]
        grouped = queries.reshape(requests, kv, group, hd)
        logits = jnp.einsum("rkgd,rktd->rkgt", grouped, k_cache, preferred_element_type=jnp.float32)
        capped = softcap * jnp.tanh(logits * query_scale / softcap)
        weights = jnp.where(is_live[:, None, None, :], jnp.exp(capped - softcap), 0.0)
        denom = direct_sum(jnp.sum(weights, axis=3))
        numer = jnp.einsum(
            "rkgt,rktd->rkgd", weights.astype(jnp.bfloat16), v_cache, preferred_element_type=jnp.float32
        )
        pieces = spread(jnp.sum(weights / denom[..., None], axis=2))
        numer = staged_sum(numer)
        attended = (numer / denom[..., None]).astype(jnp.bfloat16).reshape(requests, heads * hd)
        smem = pl.BlockSpec(memory_space=pltpu.SMEM)
        vmem = pl.BlockSpec(memory_space=pltpu.VMEM)
        mass, keep = pl.pallas_call(
            finish_kernel,
            in_specs=[smem, vmem] + [vmem] * ranks,
            out_specs=[vmem, vmem],
            out_shape=[
                jax.ShapeDtypeStruct((requests, kv, tok), jnp.float32),
                jax.ShapeDtypeStruct((requests, kv, pages), jnp.float32),
            ],
            name="finish",
        )(page_table, keep_threshold, *[pltpu.with_memory_space_constraint(p, pltpu.VMEM) for p in pieces])
        return attended, mass, keep

    return shards


def solution(mesh):
    placed = (
        P(("grp", "rep"), "head"),
        P(("grp", "rep"), "head", "seq", None),
        P(("grp", "rep"), "head", "seq", None),
        P(("grp", "rep"), None),
        P(("grp", "rep")),
        P(("grp", "rep"), "head"),
    )
    ranks = mesh.shape["seq"]
    body = program(ranks)

    return jax.shard_map(
        body,
        mesh=mesh,
        in_specs=placed,
        out_specs=(
            P(("grp", "rep"), "head"),
            P(("grp", "rep"), "head", "seq"),
            P(("grp", "rep"), "head", "seq"),
        ),
        check_vma=False,
    )
```

```python
import jax
import jax.numpy as jnp
from jax import lax
from jax.experimental import pallas as pl
from jax.experimental.pallas import tpu as pltpu
from jax.sharding import PartitionSpec as P


PAGE = 128

softcap = 50.0
query_scale = 1.0 / 12.0
quanta = 65536.0


def finish_kernel(table, threshold, *refs):
    ranks = len(refs) - 2
    pieces = refs[:ranks]
    mass, keep = refs[ranks:]
    requests, kv, tok = mass.shape
    pages = tok // PAGE
    seq = lax.axis_index("seq")
    lane = lax.broadcasted_iota(jnp.int32, (kv, pages), 1)
    eye = lax.broadcasted_iota(jnp.int32, (kv, kv), 0) == lax.broadcasted_iota(jnp.int32, (kv, kv), 1)
    for r in range(requests):
        sums = jnp.zeros((kv, pages), jnp.float32)
        for m in range(pages):
            slot = table[r, seq * pages + m]
            away = seq ^ (slot // pages)
            at = pl.multiple_of(slot % pages * PAGE, PAGE)
            page = pieces[0][r, :, pl.ds(at, PAGE)]
            for b in range(1, ranks):
                page = jnp.where(away == b, pieces[b][r, :, pl.ds(at, PAGE)], page)
            mass[r, :, m * PAGE:(m + 1) * PAGE] = page
            sums = jnp.where(lane == m, jnp.sum(page, axis=1, keepdims=True), sums)
        bar = threshold[r:r + 1, :].astype(jnp.float32)
        bar = jnp.sum(jnp.where(eye, bar, 0.0), axis=1, keepdims=True)
        keep[r] = jnp.minimum(1.0, quanta * sums / bar)


def program(ranks):
    assert ranks & (ranks - 1) == 0
    bits = [1 << b for b in reversed(range(ranks.bit_length() - 1))]

    def swap(x, bit):
        return lax.ppermute(x, "seq", [(i, i ^ bit) for i in range(ranks)])

    def direct_sum(x):
        parts = [x] + [swap(x, s) for s in range(1, ranks)]
        while len(parts) > 1:
            half = len(parts) // 2
            parts = [a + b for a, b in zip(parts[:half], parts[half:])]
        return parts[0]

    def staged_sum(x):
        for bit in bits:
            x = x + swap(x, bit)
        return x

    def spread(x):
        parts = {0: x}
        for bit in bits:
            for s, part in list(parts.items()):
                parts[s ^ bit] = swap(part, bit)
        return [parts[s] for s in range(ranks)]

    def shards(queries, k_cache, v_cache, page_table, lengths, keep_threshold):
        requests, kv, tok, hd = k_cache.shape
        heads = queries.shape[1] // hd
        group = heads // kv
        pages = tok // PAGE
        pages_all = page_table.shape[1]
        slot_ids = lax.axis_index("seq") * pages + jnp.arange(pages, dtype=jnp.int32)
        matches = page_table[:, :, None] == slot_ids[None, None, :]
        order = jnp.arange(pages_all, dtype=jnp.int32)[None, :, None]
        logical = jnp.sum(jnp.where(matches, order, 0), axis=1)
        offset = jnp.arange(PAGE, dtype=jnp.int32)[None, None, :]
        position = (logical[:, :, None] * PAGE + offset).reshape(requests, tok)
        is_live = position < lengths[:, None]
        grouped = queries.reshape(requests, kv, group, hd)
        logits = jnp.einsum("rkgd,rktd->rkgt", grouped, k_cache, preferred_element_type=jnp.float32)
        capped = softcap * jnp.tanh(logits * query_scale / softcap)
        weights = jnp.where(is_live[:, None, None, :], jnp.exp(capped - softcap), 0.0)
        denom = direct_sum(jnp.sum(weights, axis=3))
        numer = jnp.einsum(
            "rkgt,rktd->rkgd", weights.astype(jnp.bfloat16), v_cache, preferred_element_type=jnp.float32
        )
        pieces = spread(jnp.sum(weights / denom[..., None], axis=2))
        numer = staged_sum(numer)
        attended = (numer / denom[..., None]).astype(jnp.bfloat16).reshape(requests, heads * hd)
        smem = pl.BlockSpec(memory_space=pltpu.SMEM)
        vmem = pl.BlockSpec(memory_space=pltpu.VMEM)
        mass, keep = pl.pallas_call(
            finish_kernel,
            in_specs=[smem, vmem] + [vmem] * ranks,
            out_specs=[vmem, vmem],
            out_shape=[
                jax.ShapeDtypeStruct((requests, kv, tok), jnp.float32),
                jax.ShapeDtypeStruct((requests, kv, pages), jnp.float32),
            ],
            name="finish",
        )(page_table, keep_threshold, *[pltpu.with_memory_space_constraint(p, pltpu.VMEM) for p in pieces])
        return attended, mass, keep

    return shards


def solution(mesh):
    placed = (
        P(("grp", "rep"), "head"),
        P(("grp", "rep"), "head", "seq", None),
        P(("grp", "rep"), "head", "seq", None),
        P(("grp", "rep"), None),
        P(("grp", "rep")),
        P(("grp", "rep"), "head"),
    )
    ranks = mesh.shape["seq"]
    body = program(ranks)

    return jax.shard_map(
        body,
        mesh=mesh,
        in_specs=placed,
        out_specs=(
            P(("grp", "rep"), "head"),
            P(("grp", "rep"), "head", "seq"),
            P(("grp", "rep"), "head", "seq"),
        ),
        check_vma=False,
    )
```
